32 devices in a mesh: blk: 8 (over y, x, core), sub: 4 (over z).
Axes of the slice: x: 2, y: 2, z: 4, core: 2. Of those that a mesh axis runs over, the one named last changes fastest.
Arguments:
- first_core: bfloat16 [8, 128], P('blk'), may hold values from -6 to 6
- middle_core: bfloat16 [32, 32, 256], P(None, 'sub'), may hold values from -1 to 1
- last_core: bfloat16 [32, 512], replicated, may hold values from -1 to 1
- row_tt: int32 [32768], P(('blk', 'sub')), may hold values from 0 to 32767, as said below
Outputs:
- served: bfloat16 [32768, 128], P(('blk', 'sub'))
The draws below stay inside these ranges and needn't reach their ends.
Inputs may be any that keep to these rules, and one draw needn't show every extreme that they name: `row_tt`: each window row is named exactly once. Among the rows of one device, exactly 32 entries lie in each of the 32 ranges q * 1024 to (q + 1) * 1024 - 1.
All inputs are finite; a program needn't handle non-finite values.
Results may differ from the reference program's by a relative error of at most 0.0049.
Values may be sent and summed in bfloat16 or wider, within the bound.
A program may use at most 64 MiB of HBM per device.

```python
import jax
import jax.numpy as jnp
from jax import lax

R = 32
J1 = 4
J2 = 8
J3 = 4
W3 = 128
NI1 = 8
I2W = 32
ROWS_DEV = 1024
SOURCES = 32
PEER = 32


def draw_row_tt(key, part):
    spread_keys = jax.random.split(jax.random.fold_in(key, 11), SOURCES)
    spread = jax.vmap(lambda subkey: jax.random.permutation(subkey, ROWS_DEV))(spread_keys)
    spread = spread.astype(jnp.int32).reshape(SOURCES, SOURCES, PEER).transpose(1, 0, 2)
    owner_id = jnp.arange(SOURCES, dtype=jnp.int32)[None, :, None]
    flat_index = (owner_id * ROWS_DEV + spread).reshape(SOURCES, ROWS_DEV)
    shuffle_keys = jax.random.split(jax.random.fold_in(key, 12), SOURCES)
    shuffled = jax.vmap(lambda subkey, row_list: jax.random.permutation(subkey, row_list))(shuffle_keys, flat_index)
    return shuffled.reshape(-1).astype(jnp.int32)


def block_scale(stream_key, dims, cuts, least, top_value):
    def one(position, shards_of):
        draws = jax.random.uniform(jax.random.fold_in(jax.random.fold_in(stream_key, 6), position), (shards_of,), jnp.float32, least / len(cuts), top_value / len(cuts))
        return jnp.repeat(jnp.exp(draws), dims[position] // shards_of).reshape((-1,) + (1,) * (len(dims) - position - 1))

    gain = one(*cuts[0])
    for cut in cuts[1:]:
        gain = gain * one(*cut)
    return gain


def scatter_about(key, dims, scale, reach, shards=(), held_as=jnp.bfloat16):
    array = jax.random.normal(key, dims, jnp.float32) * scale
    if len(shards) > 0:
        array = block_scale(key, dims, shards, -0.22, 0.18) * array
    return jnp.clip(array, min=-reach, max=reach).astype(held_as)


def setup_inputs(seed: int = 0) -> dict:
    splits = jax.random.split(jax.random.key(seed), 5)
    return {
        "first_core": scatter_about(splits[0], (NI1, J1 * R), 1.0, 6.0, ((0, 8),)),
        "middle_core": scatter_about(splits[1], (R, I2W, J2 * R), R ** -0.5, 1.0, ((1, 4),)),
        "last_core": scatter_about(splits[2], (R, W3 * J3), R ** -0.5, 1.0),
        "row_tt": draw_row_tt(jax.random.fold_in(splits[4], 71), 0),
    }


def reference(first_core, middle_core, last_core, row_tt):
    middle_span = middle_core.shape[1]
    last_span = last_core.shape[1] // J3
    flat_middle = middle_core.reshape(R, middle_span * J2 * R)

    def slab_of(first_row):
        partial_value = jnp.dot(first_row.reshape(J1, R), flat_middle, preferred_element_type=jnp.float32).astype(jnp.bfloat16)
        partial_value = partial_value.reshape(J1, middle_span, J2, R).transpose(1, 0, 2, 3).reshape(middle_span * J1 * J2, R)
        products = jnp.dot(partial_value, last_core, preferred_element_type=jnp.float32).astype(jnp.bfloat16)
        products = products.reshape(middle_span, J1, J2, last_span, J3).transpose(0, 3, 1, 2, 4)
        return products.reshape(middle_span * last_span, J1 * J2 * J3)

    table = lax.map(slab_of, first_core)
    table = table.reshape(-1, J1 * J2 * J3)
    return jnp.take(table, row_tt.astype(jnp.int32), axis=0)
```

```python
import functools

import jax
import jax.numpy as jnp
from jax import lax
from jax.experimental import pallas as pl
from jax.experimental.pallas import tpu as pltpu
from jax.sharding import PartitionSpec as P

R = 32
J1 = 4
J2 = 8
J3 = 4
PARTIAL_LIMIT = 24 * 1024 * 1024


def exchange_rows(first_core, middle_core, last_core, row_tt):
    blocks = lax.axis_size("blk")
    groups = lax.axis_size("sub")
    sources = blocks * groups
    rows_here = row_tt.shape[0]
    per_peer = rows_here // sources
    row_width = J1 * J2 * J3
    last_span = last_core.shape[1] // J3
    middle_span = middle_core.shape[1]
    first_mat = first_core.reshape(J1, R)
    partial_value = jnp.dot(
        first_mat, middle_core.reshape(R, middle_span * J2 * R), preferred_element_type=jnp.float32
    ).astype(jnp.bfloat16)
    partial_value = (
        partial_value.reshape(J1, middle_span, J2, R)
        .transpose(1, 0, 2, 3)
        .reshape(middle_span * J1 * J2, R)
    )
    products = jnp.dot(partial_value, last_core, preferred_element_type=jnp.float32).astype(
        jnp.bfloat16
    )
    products = products.reshape(middle_span, J1, J2, last_span, J3).transpose(0, 3, 1, 2, 4)
    slab_table = products.reshape(middle_span * last_span, row_width)
    owners = row_tt // rows_here
    item_index = row_tt % rows_here
    row_order = jnp.argsort(owners, stable=True)
    wanted = item_index[row_order].reshape(blocks, groups, per_peer)
    asked_rows = lax.all_to_all(
        lax.all_to_all(wanted, "blk", split_axis=0, concat_axis=0, tiled=True),
        "sub",
        split_axis=1,
        concat_axis=1,
        tiled=True,
    )
    picked = jnp.take(slab_table, asked_rows.reshape(-1), axis=0).reshape(
        blocks, groups, per_peer, row_width
    )
    arrived = lax.all_to_all(
        lax.all_to_all(picked, "blk", split_axis=0, concat_axis=0, tiled=True),
        "sub",
        split_axis=1,
        concat_axis=1,
        tiled=True,
    )
    gathered = arrived.reshape(rows_here, row_width)
    return jnp.take(gathered, jnp.argsort(row_order), axis=0)


def iota(shape, axis):
    return lax.broadcasted_iota(jnp.int32, shape, axis)


def fill_last(last_ref, spread_ref):
    width = J1 * J2 * J3
    tiles = last_ref.shape[1] // width
    per_tile = width // J3
    stacked = jnp.concatenate(
        [last_ref[:, t * width : (t + 1) * width] for t in range(tiles)], axis=0
    )
    for pair in range(per_tile // 2):
        lane = iota((width, 2 * width), 1)
        want = (2 * pair + lane // width) * J3 + lane % J3
        pick = jnp.where(iota((width, 2 * width), 0) == want, 1.0, 0.0).astype(jnp.bfloat16)
        both = jnp.dot(stacked, pick, preferred_element_type=jnp.float32)
        for t in range(tiles):
            for half in range(2):
                spread_ref[t * per_tile + 2 * pair + half] = both[
                    t * R : (t + 1) * R, half * width : (half + 1) * width
                ]


def fill_first(rows, wide_ref):
    width = J1 * J2 * J3
    lane = iota((R, width), 1)
    own = lane % R == iota((R, width), 0)
    spread = jnp.concatenate(
        [jnp.where(own, jnp.broadcast_to(row, (R, width)), 0.0) for row in rows], axis=0
    ).astype(jnp.bfloat16)
    lane_of = iota((J1 * R, width), 1) // (J2 * J3)
    same = jnp.where(iota((J1 * R, width), 0) // R == lane_of, 1.0, 0.0).astype(jnp.bfloat16)
    wide = jnp.dot(spread, same, preferred_element_type=jnp.float32)
    for i in range(len(rows)):
        block = wide[i * R : (i + 1) * R]
        for j in range(J2):
            kept = jnp.where(lane // J3 % J2 == j, block, 0.0)
            wide_ref[j * R : (j + 1) * R, i * width : (i + 1) * width] = kept.astype(jnp.bfloat16)


def fill_partial(group, middle, wide_ref, partial_ref, middle_all):
    width = J1 * J2 * J3
    span = middle.shape[0] // R
    found = jnp.dot(middle, wide_ref[...], preferred_element_type=jnp.float32)
    found = found.astype(jnp.bfloat16).astype(jnp.float32)
    for i in range(wide_ref.shape[1] // width):
        for m in range(span):
            partial_ref[i * middle_all + group * span + m] = found[
                m * R : (m + 1) * R, i * width : (i + 1) * width
            ]


def serve(row_ref, partial_ref, spread_ref, sums_ref, out_ref):
    rows_here, width = out_ref.shape
    last_span = spread_ref.shape[0]
    parts = R // 8
    unroll = 16

    def some_rows(step, carry):
        for u in range(unroll):
            k = step * unroll + u
            row = row_ref[k]
            left = partial_ref[row // last_span]
            right = spread_ref[row % last_span]
            product = left * right
            total = product[0:8]
            for p in range(1, parts):
                total = total + product[8 * p : 8 * p + 8]
            sums_ref[pl.ds(pl.multiple_of(k * 8, 8), 8), :] = total
        return carry

    lax.fori_loop(0, rows_here // unroll, some_rows, 0)
    chunk = 128

    def some_sums(step, carry):
        base = pl.multiple_of(step * chunk * 8, chunk * 8)
        total = sums_ref[pl.ds(base, chunk, stride=8), :]
        for s in range(1, 8):
            total = total + sums_ref[pl.ds(base + s, chunk, stride=8), :]
        out_ref[pl.ds(pl.multiple_of(step * chunk, chunk), chunk), :] = total.astype(out_ref.dtype)
        return carry

    lax.fori_loop(0, rows_here // chunk, some_sums, 0)


def build(groups, row_ref, first_ref, middle_ref, last_ref, out_ref, wide_ref, partial_ref, spread_ref, sums_ref):
    fill_last(last_ref, spread_ref)
    first = first_ref[...].astype(jnp.float32)
    fill_first([first[i : i + 1] for i in range(first.shape[0])], wide_ref)
    part = middle_ref.shape[0] // groups
    for g in range(groups):
        fill_partial(
            g, middle_ref[g * part : (g + 1) * part, :], wide_ref, partial_ref, middle_ref.shape[0] // R
        )
    serve(row_ref, partial_ref, spread_ref, sums_ref, out_ref)


def rebuild_rows(first_core, middle_core, last_core, row_tt):
    blocks = lax.axis_size("blk")
    groups = lax.axis_size("sub")
    width = J1 * J2 * J3
    rows_here = row_tt.shape[0]
    span = middle_core.shape[1]
    last_span = last_core.shape[1] // J3
    turned = middle_core.reshape(R, span, J2, R).transpose(1, 3, 2, 0).reshape(span * R, J2 * R)
    middle_all = lax.all_gather(turned, "sub", axis=0, tiled=True)
    first_all = lax.all_gather(first_core, "blk", axis=0, tiled=True)
    vmem = pl.BlockSpec(memory_space=pltpu.VMEM)
    return pl.pallas_call(
        functools.partial(build, groups),
        out_shape=jax.ShapeDtypeStruct((rows_here, width), jnp.bfloat16),
        in_specs=[pl.BlockSpec(memory_space=pltpu.SMEM), vmem, vmem, vmem],
        out_specs=vmem,
        scratch_shapes=[
            pltpu.VMEM((J2 * R, blocks * width), jnp.bfloat16),
            pltpu.VMEM((blocks * groups * span, R, width), jnp.float32),
            pltpu.VMEM((last_span, R, width), jnp.float32),
            pltpu.VMEM((rows_here * 8, width), jnp.float32),
        ],
    )(row_tt, first_all, middle_all, last_core)


def on_device(first_core, middle_core, last_core, row_tt):
    indices = lax.axis_size("blk") * lax.axis_size("sub") * middle_core.shape[1]
    if indices * R * J1 * J2 * J3 * 4 > PARTIAL_LIMIT:
        return exchange_rows(first_core, middle_core, last_core, row_tt)
    return rebuild_rows(first_core, middle_core, last_core, row_tt)


def solution(mesh):
    placed = (P("blk", None), P(None, "sub", None), P(), P(("blk", "sub")))
    return jax.shard_map(
        on_device, mesh=mesh, in_specs=placed, out_specs=P(("blk", "sub"), None), check_vma=False
    )
```

```python
import functools

import jax
import jax.numpy as jnp
from jax import lax
from jax.experimental import pallas as pl
from jax.experimental.pallas import tpu as pltpu
from jax.sharding import PartitionSpec as P

R = 32
J1 = 4
J2 = 8
J3 = 4
PARTIAL_LIMIT = 24 * 1024 * 1024
MESH = pl.DeviceIdType.MESH


def exchange_rows(first_core, middle_core, last_core, row_tt):
    blocks = lax.axis_size("blk")
    groups = lax.axis_size("sub")
    sources = blocks * groups
    rows_here = row_tt.shape[0]
    per_peer = rows_here // sources
    row_width = J1 * J2 * J3
    last_span = last_core.shape[1] // J3
    middle_span = middle_core.shape[1]
    first_mat = first_core.reshape(J1, R)
    partial_value = jnp.dot(
        first_mat, middle_core.reshape(R, middle_span * J2 * R), preferred_element_type=jnp.float32
    ).astype(jnp.bfloat16)
    partial_value = (
        partial_value.reshape(J1, middle_span, J2, R)
        .transpose(1, 0, 2, 3)
        .reshape(middle_span * J1 * J2, R)
    )
    products = jnp.dot(partial_value, last_core, preferred_element_type=jnp.float32).astype(
        jnp.bfloat16
    )
    products = products.reshape(middle_span, J1, J2, last_span, J3).transpose(0, 3, 1, 2, 4)
    slab_table = products.reshape(middle_span * last_span, row_width)
    owners = row_tt // rows_here
    item_index = row_tt % rows_here
    row_order = jnp.argsort(owners, stable=True)
    wanted = item_index[row_order].reshape(blocks, groups, per_peer)
    asked_rows = lax.all_to_all(
        lax.all_to_all(wanted, "blk", split_axis=0, concat_axis=0, tiled=True),
        "sub",
        split_axis=1,
        concat_axis=1,
        tiled=True,
    )
    picked = jnp.take(slab_table, asked_rows.reshape(-1), axis=0).reshape(
        blocks, groups, per_peer, row_width
    )
    arrived = lax.all_to_all(
        lax.all_to_all(picked, "blk", split_axis=0, concat_axis=0, tiled=True),
        "sub",
        split_axis=1,
        concat_axis=1,
        tiled=True,
    )
    gathered = arrived.reshape(rows_here, row_width)
    return jnp.take(gathered, jnp.argsort(row_order), axis=0)


def iota(shape, axis):
    return lax.broadcasted_iota(jnp.int32, shape, axis)


def fill_last(last_ref, spread_ref):
    width = J1 * J2 * J3
    tiles = last_ref.shape[1] // width
    per_tile = width // J3
    stacked = jnp.concatenate(
        [last_ref[:, t * width : (t + 1) * width] for t in range(tiles)], axis=0
    )
    for pair in range(per_tile // 2):
        lane = iota((width, 2 * width), 1)
        want = (2 * pair + lane // width) * J3 + lane % J3
        pick = jnp.where(iota((width, 2 * width), 0) == want, 1.0, 0.0).astype(jnp.bfloat16)
        both = jnp.dot(stacked, pick, preferred_element_type=jnp.float32)
        for t in range(tiles):
            for half in range(2):
                spread_ref[t * per_tile + 2 * pair + half] = both[
                    t * R : (t + 1) * R, half * width : (half + 1) * width
                ]


def fill_first(rows, wide_ref):
    width = J1 * J2 * J3
    lane = iota((R, width), 1)
    own = lane % R == iota((R, width), 0)
    spread = jnp.concatenate(
        [jnp.where(own, jnp.broadcast_to(row, (R, width)), 0.0) for row in rows], axis=0
    ).astype(jnp.bfloat16)
    lane_of = iota((J1 * R, width), 1) // (J2 * J3)
    same = jnp.where(iota((J1 * R, width), 0) // R == lane_of, 1.0, 0.0).astype(jnp.bfloat16)
    wide = jnp.dot(spread, same, preferred_element_type=jnp.float32)
    for i in range(len(rows)):
        block = wide[i * R : (i + 1) * R]
        for j in range(J2):
            kept = jnp.where(lane // J3 % J2 == j, block, 0.0)
            wide_ref[j * R : (j + 1) * R, i * width : (i + 1) * width] = kept.astype(jnp.bfloat16)


def fill_partial(group, middle, wide_ref, partial_ref, middle_all):
    width = J1 * J2 * J3
    span = middle.shape[0] // R
    found = jnp.dot(middle, wide_ref[...], preferred_element_type=jnp.float32)
    found = found.astype(jnp.bfloat16).astype(jnp.float32)
    for i in range(wide_ref.shape[1] // width):
        for m in range(span):
            partial_ref[i * middle_all + group * span + m] = found[
                m * R : (m + 1) * R, i * width : (i + 1) * width
            ]


def serve(row_ref, partial_ref, spread_ref, sums_ref, out_ref):
    rows_here, width = out_ref.shape
    last_span = spread_ref.shape[0]
    shift = last_span.bit_length() - 1
    parts = R // 8
    unroll = 16

    def some_rows(step, carry):
        for u in range(unroll):
            k = step * unroll + u
            row = row_ref[k]
            left = partial_ref[lax.shift_right_logical(row, shift)]
            right = spread_ref[row & (last_span - 1)]
            product = left * right
            total = product[0:8]
            for p in range(1, parts):
                total = total + product[8 * p : 8 * p + 8]
            sums_ref[pl.ds(pl.multiple_of(k * 8, 8), 8), :] = total
        return carry

    lax.fori_loop(0, rows_here // unroll, some_rows, 0)
    chunk = 128

    def some_sums(step, carry):
        base = pl.multiple_of(step * chunk * 8, chunk * 8)
        total = sums_ref[pl.ds(base, chunk, stride=8), :]
        for s in range(1, 8):
            total = total + sums_ref[pl.ds(base + s, chunk, stride=8), :]
        out_ref[pl.ds(pl.multiple_of(step * chunk, chunk), chunk), :] = total.astype(out_ref.dtype)
        return carry

    lax.fori_loop(0, rows_here // chunk, some_sums, 0)


def turn(middle, span):
    rows = middle.shape[0]
    here, there = iota((rows, rows), 0), iota((rows, rows), 1)
    same = (here // span == there % R) & (here % span == there // R)
    order = jnp.where(same, 1.0, 0.0).astype(jnp.bfloat16)
    flipped = lax.dot_general(
        middle, order, (((0,), (0,)), ((), ())), preferred_element_type=jnp.float32
    )
    strips = []
    for m in range(span):
        strips.append(
            jnp.concatenate(
                [flipped[j * R : (j + 1) * R, m * R : (m + 1) * R] for j in range(J2)], axis=1
            )
        )
    return jnp.concatenate(strips, axis=0).astype(jnp.bfloat16)


def build(
    blocks,
    groups,
    row_ref,
    first_ref,
    middle_ref,
    last_ref,
    out_ref,
    first_all,
    middle_all,
    wide_ref,
    partial_ref,
    spread_ref,
    sums_ref,
    first_send,
    first_recv,
    far_send,
    far_recv,
    near_send,
    near_recv,
):
    blk = lax.axis_index("blk")
    sub = lax.axis_index("sub")
    rows = middle_ref.shape[0]
    span = rows // R
    half = rows // 2
    side = blk % 2
    partner = blk + 1 - 2 * side
    barrier = pltpu.get_barrier_semaphore()
    for d in range(1, blocks):
        pl.semaphore_signal(
            barrier, inc=1, device_id=((blk + d) % blocks, sub), device_id_type=MESH
        )
    for d in range(1, groups):
        pl.semaphore_signal(
            barrier, inc=1, device_id=(blk, (sub + d) % groups), device_id_type=MESH
        )
    middle_all[sub] = turn(middle_ref[...], span)
    first_all[blk] = first_ref[...]
    pl.semaphore_wait(barrier, blocks + groups - 2)

    def half_of(source, which):
        return middle_all.at[source, pl.ds(pl.multiple_of(which * half, half), half)]

    far = {}
    for d in (2, 1, 3) if groups == 4 else range(1, groups):
        far[d] = pltpu.make_async_remote_copy(
            src_ref=half_of(sub, side),
            dst_ref=half_of(sub, side),
            send_sem=far_send.at[d - 1],
            recv_sem=far_recv.at[d - 1],
            device_id=(blk, (sub + d) % groups),
            device_id_type=MESH,
        )
        far[d].start()
    firsts = []
    for d in range(1, blocks):
        copy = pltpu.make_async_remote_copy(
            src_ref=first_ref,
            dst_ref=first_all.at[blk],
            send_sem=first_send.at[d - 1],
            recv_sem=first_recv.at[d - 1],
            device_id=((blk + d) % blocks, sub),
            device_id_type=MESH,
        )
        copy.start()
        firsts.append(copy)
    fill_last(last_ref, spread_ref)
    for copy in firsts:
        copy.wait_recv()
    first = [first_all[i].astype(jnp.float32) for i in range(blocks)]
    fill_first(first, wide_ref)
    fill_partial(sub, middle_all[sub], wide_ref, partial_ref, groups * span)
    near = {}
    order = [1, 3, 2] if groups == 4 else list(range(1, groups))
    for d in order:
        source = (sub - d + groups) % groups
        pltpu.make_async_remote_copy(
            src_ref=half_of(sub, side),
            dst_ref=half_of(source, side),
            send_sem=far_send.at[d - 1],
            recv_sem=far_recv.at[d - 1],
            device_id=(blk, (sub + d) % groups),
            device_id_type=MESH,
        ).wait_recv()
        near[d] = pltpu.make_async_remote_copy(
            src_ref=half_of(source, side),
            dst_ref=half_of(source, side),
            send_sem=near_send.at[d - 1],
            recv_sem=near_recv.at[d - 1],
            device_id=(partner, sub),
            device_id_type=MESH,
        )
        near[d].start()
    for d in order:
        source = (sub - d + groups) % groups
        near[d].wait_recv()
        fill_partial(source, middle_all[source], wide_ref, partial_ref, groups * span)
    serve(row_ref, partial_ref, spread_ref, sums_ref, out_ref)
    for copy in firsts + list(far.values()) + list(near.values()):
        copy.wait_send()


def rebuild_rows(first_core, middle_core, last_core, row_tt):
    blocks = lax.axis_size("blk")
    groups = lax.axis_size("sub")
    width = J1 * J2 * J3
    rows_here = row_tt.shape[0]
    span = middle_core.shape[1]
    last_span = last_core.shape[1] // J3
    vmem = pl.BlockSpec(memory_space=pltpu.VMEM)
    return pl.pallas_call(
        functools.partial(build, blocks, groups),
        out_shape=jax.ShapeDtypeStruct((rows_here, width), jnp.bfloat16),
        in_specs=[pl.BlockSpec(memory_space=pltpu.SMEM), vmem, vmem, vmem],
        out_specs=vmem,
        scratch_shapes=[
            pltpu.VMEM((blocks, 1, J1 * R), jnp.bfloat16),
            pltpu.VMEM((groups, span * R, J2 * R), jnp.bfloat16),
            pltpu.VMEM((J2 * R, blocks * width), jnp.bfloat16),
            pltpu.VMEM((blocks * groups * span, R, width), jnp.float32),
            pltpu.VMEM((last_span, R, width), jnp.float32),
            pltpu.VMEM((rows_here * 8, width), jnp.float32),
            pltpu.SemaphoreType.DMA((blocks - 1,)),
            pltpu.SemaphoreType.DMA((blocks - 1,)),
            pltpu.SemaphoreType.DMA((groups - 1,)),
            pltpu.SemaphoreType.DMA((groups - 1,)),
            pltpu.SemaphoreType.DMA((groups - 1,)),
            pltpu.SemaphoreType.DMA((groups - 1,)),
        ],
        compiler_params=pltpu.CompilerParams(collective_id=0, has_side_effects=True),
    )(row_tt, first_core, middle_core.reshape(R * span, J2 * R), last_core)


def on_device(first_core, middle_core, last_core, row_tt):
    blocks = lax.axis_size("blk")
    indices = blocks * lax.axis_size("sub") * middle_core.shape[1]
    last_span = last_core.shape[1] // J3
    small = indices * R * J1 * J2 * J3 * 4 <= PARTIAL_LIMIT
    if not small or blocks % 2 or last_span & (last_span - 1):
        return exchange_rows(first_core, middle_core, last_core, row_tt)
    return rebuild_rows(first_core, middle_core, last_core, row_tt)


def solution(mesh):
    placed = (P("blk", None), P(None, "sub", None), P(), P(("blk", "sub")))
    return jax.shard_map(
        on_device, mesh=mesh, in_specs=placed, out_specs=P(("blk", "sub"), None), check_vma=False
    )
```

```python
import functools

import jax
import jax.numpy as jnp
from jax import lax
from jax.experimental import pallas as pl
from jax.experimental.pallas import tpu as pltpu
from jax.sharding import PartitionSpec as P

R = 32
J1 = 4
J2 = 8
J3 = 4
PARTIAL_LIMIT = 24 * 1024 * 1024
MESH = pl.DeviceIdType.MESH


def exchange_rows(first_core, middle_core, last_core, row_tt):
    blocks = lax.axis_size("blk")
    groups = lax.axis_size("sub")
    sources = blocks * groups
    rows_here = row_tt.shape[0]
    per_peer = rows_here // sources
    row_width = J1 * J2 * J3
    last_span = last_core.shape[1] // J3
    middle_span = middle_core.shape[1]
    first_mat = first_core.reshape(J1, R)
    partial_value = jnp.dot(
        first_mat, middle_core.reshape(R, middle_span * J2 * R), preferred_element_type=jnp.float32
    ).astype(jnp.bfloat16)
    partial_value = (
        partial_value.reshape(J1, middle_span, J2, R)
        .transpose(1, 0, 2, 3)
        .reshape(middle_span * J1 * J2, R)
    )
    products = jnp.dot(partial_value, last_core, preferred_element_type=jnp.float32).astype(
        jnp.bfloat16
    )
    products = products.reshape(middle_span, J1, J2, last_span, J3).transpose(0, 3, 1, 2, 4)
    slab_table = products.reshape(middle_span * last_span, row_width)
    owners = row_tt // rows_here
    item_index = row_tt % rows_here
    row_order = jnp.argsort(owners, stable=True)
    wanted = item_index[row_order].reshape(blocks, groups, per_peer)
    asked_rows = lax.all_to_all(
        lax.all_to_all(wanted, "blk", split_axis=0, concat_axis=0, tiled=True),
        "sub",
        split_axis=1,
        concat_axis=1,
        tiled=True,
    )
    picked = jnp.take(slab_table, asked_rows.reshape(-1), axis=0).reshape(
        blocks, groups, per_peer, row_width
    )
    arrived = lax.all_to_all(
        lax.all_to_all(picked, "blk", split_axis=0, concat_axis=0, tiled=True),
        "sub",
        split_axis=1,
        concat_axis=1,
        tiled=True,
    )
    gathered = arrived.reshape(rows_here, row_width)
    return jnp.take(gathered, jnp.argsort(row_order), axis=0)


def iota(shape, axis):
    return lax.broadcasted_iota(jnp.int32, shape, axis)


def fill_last(last_ref, spread_ref):
    width = J1 * J2 * J3
    tiles = last_ref.shape[1] // width
    per_tile = width // J3
    stacked = jnp.concatenate(
        [last_ref[:, t * width : (t + 1) * width] for t in range(tiles)], axis=0
    )
    for pair in range(per_tile // 2):
        lane = iota((width, 2 * width), 1)
        want = (2 * pair + lane // width) * J3 + lane % J3
        pick = jnp.where(iota((width, 2 * width), 0) == want, 1.0, 0.0).astype(jnp.bfloat16)
        both = jnp.dot(stacked, pick, preferred_element_type=jnp.float32)
        for t in range(tiles):
            for half in range(2):
                spread_ref[t * per_tile + 2 * pair + half] = both[
                    t * R : (t + 1) * R, half * width : (half + 1) * width
                ]


def fill_first(rows, wide_ref):
    width = J1 * J2 * J3
    lane = iota((R, width), 1)
    own = lane % R == iota((R, width), 0)
    spread = jnp.concatenate(
        [jnp.where(own, jnp.broadcast_to(row, (R, width)), 0.0) for row in rows], axis=0
    ).astype(jnp.bfloat16)
    lane_of = iota((J1 * R, width), 1) // (J2 * J3)
    same = jnp.where(iota((J1 * R, width), 0) // R == lane_of, 1.0, 0.0).astype(jnp.bfloat16)
    wide = jnp.dot(spread, same, preferred_element_type=jnp.float32)
    for i in range(len(rows)):
        block = wide[i * R : (i + 1) * R]
        for j in range(J2):
            kept = jnp.where(lane // J3 % J2 == j, block, 0.0)
            wide_ref[j * R : (j + 1) * R, i * width : (i + 1) * width] = kept.astype(jnp.bfloat16)


def fill_partial(group, middle, wide_ref, partial_ref, middle_all):
    width = J1 * J2 * J3
    span = middle.shape[0] // R
    found = jnp.dot(middle, wide_ref[...], preferred_element_type=jnp.float32)
    found = found.astype(jnp.bfloat16).astype(jnp.float32)
    for i in range(wide_ref.shape[1] // width):
        for m in range(span):
            partial_ref[i * middle_all + group * span + m] = found[
                m * R : (m + 1) * R, i * width : (i + 1) * width
            ]


def serve(row_ref, partial_ref, spread_ref, sums_ref, out_ref):
    rows_here, width = out_ref.shape
    last_span = spread_ref.shape[0]
    shift = last_span.bit_length() - 1
    parts = R // 8
    unroll = 16

    def some_rows(step, carry):
        for u in range(unroll):
            k = step * unroll + u
            row = row_ref[k]
            left = partial_ref[lax.shift_right_logical(row, shift)]
            right = spread_ref[row & (last_span - 1)]
            product = left * right
            total = product[0:8]
            for p in range(1, parts):
                total = total + product[8 * p : 8 * p + 8]
            sums_ref[pl.ds(pl.multiple_of(k * 8, 8), 8), :] = total
        return carry

    lax.fori_loop(0, rows_here // unroll, some_rows, 0)
    chunk = 128

    def some_sums(step, carry):
        base = pl.multiple_of(step * chunk * 8, chunk * 8)
        total = sums_ref[pl.ds(base, chunk, stride=8), :]
        for s in range(1, 8):
            total = total + sums_ref[pl.ds(base + s, chunk, stride=8), :]
        out_ref[pl.ds(pl.multiple_of(step * chunk, chunk), chunk), :] = total.astype(out_ref.dtype)
        return carry

    lax.fori_loop(0, rows_here // chunk, some_sums, 0)


def turn(middle, span):
    rows = middle.shape[0]
    here, there = iota((rows, rows), 0), iota((rows, rows), 1)
    same = (here // span == there % R) & (here % span == there // R)
    order = jnp.where(same, 1.0, 0.0).astype(jnp.bfloat16)
    flipped = lax.dot_general(
        middle, order, (((0,), (0,)), ((), ())), preferred_element_type=jnp.float32
    )
    strips = []
    for m in range(span):
        strips.append(
            jnp.concatenate(
                [flipped[j * R : (j + 1) * R, m * R : (m + 1) * R] for j in range(J2)], axis=1
            )
        )
    return jnp.concatenate(strips, axis=0).astype(jnp.bfloat16)


def build(
    blocks,
    groups,
    row_ref,
    first_ref,
    middle_ref,
    last_ref,
    out_ref,
    first_all,
    middle_all,
    wide_ref,
    partial_ref,
    spread_ref,
    sums_ref,
    first_send,
    first_recv,
    far_send,
    far_recv,
    near_send,
    near_recv,
):
    blk = lax.axis_index("blk")
    sub = lax.axis_index("sub")
    rows = middle_ref.shape[0]
    span = rows // R
    half = rows // 2
    side = blk % 2
    partner = blk + 1 - 2 * side
    barrier = pltpu.get_barrier_semaphore()
    for d in range(1, blocks):
        pl.semaphore_signal(
            barrier, inc=1, device_id=((blk + d) % blocks, sub), device_id_type=MESH
        )
    for d in range(1, groups):
        pl.semaphore_signal(
            barrier, inc=1, device_id=(blk, (sub + d) % groups), device_id_type=MESH
        )
    middle_all[sub] = turn(middle_ref[...], span)
    first_all[blk] = first_ref[...]
    pl.semaphore_wait(barrier, blocks + groups - 2)

    def half_of(source, which):
        return middle_all.at[source, pl.ds(pl.multiple_of(which * half, half), half)]

    far = {}
    for d in (2, 1, 3) if groups == 4 else range(1, groups):
        far[d] = pltpu.make_async_remote_copy(
            src_ref=half_of(sub, side),
            dst_ref=half_of(sub, side),
            send_sem=far_send.at[d - 1],
            recv_sem=far_recv.at[d - 1],
            device_id=(blk, (sub + d) % groups),
            device_id_type=MESH,
        )
        far[d].start()
    firsts = []
    for d in range(1, blocks):
        copy = pltpu.make_async_remote_copy(
            src_ref=first_ref,
            dst_ref=first_all.at[blk],
            send_sem=first_send.at[d - 1],
            recv_sem=first_recv.at[d - 1],
            device_id=((blk + d) % blocks, sub),
            device_id_type=MESH,
        )
        copy.start()
        firsts.append(copy)
    fill_last(last_ref, spread_ref)
    for copy in firsts:
        copy.wait_recv()
    first = [first_all[i].astype(jnp.float32) for i in range(blocks)]
    fill_first(first, wide_ref)
    fill_partial(sub, middle_all[sub], wide_ref, partial_ref, groups * span)
    near = {}
    order = [1, 3, 2] if groups == 4 else list(range(1, groups))
    for d in order:
        source = (sub - d + groups) % groups
        pltpu.make_async_remote_copy(
            src_ref=half_of(sub, side),
            dst_ref=half_of(source, side),
            send_sem=far_send.at[d - 1],
            recv_sem=far_recv.at[d - 1],
            device_id=(blk, (sub + d) % groups),
            device_id_type=MESH,
        ).wait_recv()
        near[d] = pltpu.make_async_remote_copy(
            src_ref=half_of(source, side),
            dst_ref=half_of(source, side),
            send_sem=near_send.at[d - 1],
            recv_sem=near_recv.at[d - 1],
            device_id=(partner, sub),
            device_id_type=MESH,
        )
        near[d].start()
    for d in order:
        source = (sub - d + groups) % groups
        near[d].wait_recv()
        fill_partial(source, middle_all[source], wide_ref, partial_ref, groups * span)
    serve(row_ref, partial_ref, spread_ref, sums_ref, out_ref)
    for copy in firsts + list(far.values()) + list(near.values()):
        copy.wait_send()


def rebuild_rows(first_core, middle_core, last_core, row_tt):
    blocks = lax.axis_size("blk")
    groups = lax.axis_size("sub")
    width = J1 * J2 * J3
    rows_here = row_tt.shape[0]
    span = middle_core.shape[1]
    last_span = last_core.shape[1] // J3
    vmem = pl.BlockSpec(memory_space=pltpu.VMEM)
    return pl.pallas_call(
        functools.partial(build, blocks, groups),
        out_shape=pltpu.VMEM((rows_here, width), jnp.bfloat16),
        in_specs=[pl.BlockSpec(memory_space=pltpu.SMEM), vmem, vmem, vmem],
        out_specs=vmem,
        scratch_shapes=[
            pltpu.VMEM((blocks, 1, J1 * R), jnp.bfloat16),
            pltpu.VMEM((groups, span * R, J2 * R), jnp.bfloat16),
            pltpu.VMEM((J2 * R, blocks * width), jnp.bfloat16),
            pltpu.VMEM((blocks * groups * span, R, width), jnp.float32),
            pltpu.VMEM((last_span, R, width), jnp.float32),
            pltpu.VMEM((rows_here * 8, width), jnp.float32),
            pltpu.SemaphoreType.DMA((blocks - 1,)),
            pltpu.SemaphoreType.DMA((blocks - 1,)),
            pltpu.SemaphoreType.DMA((groups - 1,)),
            pltpu.SemaphoreType.DMA((groups - 1,)),
            pltpu.SemaphoreType.DMA((groups - 1,)),
            pltpu.SemaphoreType.DMA((groups - 1,)),
        ],
        compiler_params=pltpu.CompilerParams(collective_id=0, has_side_effects=True),
    )(row_tt, first_core, middle_core.reshape(R * span, J2 * R), last_core)


def on_device(first_core, middle_core, last_core, row_tt):
    blocks = lax.axis_size("blk")
    indices = blocks * lax.axis_size("sub") * middle_core.shape[1]
    last_span = last_core.shape[1] // J3
    small = indices * R * J1 * J2 * J3 * 4 <= PARTIAL_LIMIT
    if not small or blocks % 2 or last_span & (last_span - 1):
        return exchange_rows(first_core, middle_core, last_core, row_tt)
    return rebuild_rows(first_core, middle_core, last_core, row_tt)


def solution(mesh):
    placed = (P("blk", None), P(None, "sub", None), P(), P(("blk", "sub")))
    return jax.shard_map(
        on_device, mesh=mesh, in_specs=placed, out_specs=P(("blk", "sub"), None), check_vma=False
    )
```
